32 devices in a mesh: dp: 1 (over z), ep: 32 (over y, x, core).
Axes of the slice: x: 4, y: 4, z: 1, core: 2. Of those that a mesh axis runs over, the one named last changes fastest.
The devices are a block of a 4x4x8 slice.
Arguments:
- tokens_a: bfloat16 [16384, 2048], P(('dp', 'ep'))
- experts_a: int32 [16384, 8], P(('dp', 'ep'))
- slots_a: int32 [16384, 8], P(('dp', 'ep'))
- gates_a: bfloat16 [16384, 8], P(('dp', 'ep'))
- tokens_b: bfloat16 [16384, 2048], P(('dp', 'ep'))
- experts_b: int32 [16384, 8], P(('dp', 'ep'))
- slots_b: int32 [16384, 8], P(('dp', 'ep'))
- gates_b: bfloat16 [16384, 8], P(('dp', 'ep'))
- attn_gain: bfloat16 [2048], replicated
- w_query: bfloat16 [2048, 16, 128], replicated
- w_key: bfloat16 [2048, 16, 128], replicated
- w_value: bfloat16 [2048, 16, 128], replicated
- w_out: bfloat16 [16, 128, 2048], replicated
- moe_gain: bfloat16 [2048], replicated
- w_gate: bfloat16 [64, 2048, 1024], P('ep')
- w_up: bfloat16 [64, 2048, 1024], P('ep')
- w_down: bfloat16 [64, 1024, 2048], P('ep')
Outputs:
- output 1: bfloat16 [16384, 2048], P(('dp', 'ep'))
- output 2: bfloat16 [16384, 2048], P(('dp', 'ep'))
All inputs are finite; a program needn't handle non-finite values.
Results may differ from the reference program's by a relative error of at most 0.0130805.
Values are sent between devices in bfloat16 or wider.
A program may use at most 768 MiB of HBM per device.

```python
import jax
import jax.numpy as jnp
from jax import lax

MODEL_DIM = 2048
FFN_DIM = 1024
EXPERTS = 64
TOP_K = 8
HEADS = 16
TOKENS = 512
GROUP = 32
SLOTS = 128

HEAD_DIM = MODEL_DIM // HEADS
ROWS = GROUP * TOKENS
NORM_EPS = 1e-6
MASK_VALUE = -1e30


def draw_routing(route_key):
    key_start, key_hot, key_pick = jax.random.split(route_key, 3)
    spacing = EXPERTS // TOP_K
    hot_span = max(1, EXPERTS // (4 * TOP_K))
    start_any = jax.random.randint(key_start, (ROWS,), 0, EXPERTS)
    start_hot = jax.random.randint(key_hot, (ROWS,), 0, hot_span)
    use_hot = jax.random.randint(key_pick, (ROWS,), 0, 2) == 1
    position = jnp.arange(ROWS) % TOKENS
    first_expert = jnp.where(use_hot, start_hot, start_any)
    first_expert = jnp.where(position <= SLOTS, 0, first_expert)
    choice = (first_expert[:, None] + spacing * jnp.arange(TOP_K)[None, :]) % EXPERTS
    choice = choice.astype(jnp.int32)

    def device_slots(dev_choice):
        flat_ids = dev_choice.reshape(-1)
        onehot = (flat_ids[:, None] == jnp.arange(EXPERTS)[None, :]).astype(jnp.int32)
        rank_pos = jnp.sum(jnp.cumsum(onehot, axis=0) * onehot, axis=1) - 1
        return jnp.where(rank_pos < SLOTS, rank_pos, -1).reshape(TOKENS, TOP_K)

    slot_ids = lax.map(device_slots, choice.reshape(GROUP, TOKENS, TOP_K))
    return choice, slot_ids.reshape(ROWS, TOP_K).astype(jnp.int32)


def setup_inputs(seed: int = 0, part: int = 0) -> dict:
    base_key = jax.random.key(seed)
    part_key = jax.random.fold_in(base_key, part)
    part_keys = jax.random.split(part_key, 6)
    shared_keys = jax.random.split(base_key, 9)
    scale_in = MODEL_DIM ** -0.5
    scale_ffn = FFN_DIM ** -0.5
    experts_a, slots_a = draw_routing(part_keys[1])
    experts_b, slots_b = draw_routing(part_keys[4])
    return {
        "tokens_a": jax.random.normal(part_keys[0], (ROWS, MODEL_DIM), jnp.float32).astype(jnp.bfloat16),
        "experts_a": experts_a,
        "slots_a": slots_a,
        "gates_a": jax.random.uniform(part_keys[2], (ROWS, TOP_K), jnp.float32, 0.5, 1.5).astype(jnp.bfloat16),
        "tokens_b": jax.random.normal(part_keys[3], (ROWS, MODEL_DIM), jnp.float32).astype(jnp.bfloat16),
        "experts_b": experts_b,
        "slots_b": slots_b,
        "gates_b": jax.random.uniform(part_keys[5], (ROWS, TOP_K), jnp.float32, 0.5, 1.5).astype(jnp.bfloat16),
        "attn_gain": (1.0 + 0.3 * jax.random.normal(shared_keys[0], (MODEL_DIM,), jnp.float32)).astype(jnp.bfloat16),
        "w_query": (1.5 * scale_in * jax.random.normal(shared_keys[1], (MODEL_DIM, HEADS, HEAD_DIM), jnp.float32)).astype(jnp.bfloat16),
        "w_key": (1.5 * scale_in * jax.random.normal(shared_keys[2], (MODEL_DIM, HEADS, HEAD_DIM), jnp.float32)).astype(jnp.bfloat16),
        "w_value": (scale_in * jax.random.normal(shared_keys[3], (MODEL_DIM, HEADS, HEAD_DIM), jnp.float32)).astype(jnp.bfloat16),
        "w_out": (scale_in * jax.random.normal(shared_keys[4], (HEADS, HEAD_DIM, MODEL_DIM), jnp.float32)).astype(jnp.bfloat16),
        "moe_gain": (1.0 + 0.3 * jax.random.normal(shared_keys[5], (MODEL_DIM,), jnp.float32)).astype(jnp.bfloat16),
        "w_gate": (scale_in * jax.random.normal(shared_keys[6], (EXPERTS, MODEL_DIM, FFN_DIM), jnp.float32)).astype(jnp.bfloat16),
        "w_up": (scale_in * jax.random.normal(shared_keys[7], (EXPERTS, MODEL_DIM, FFN_DIM), jnp.float32)).astype(jnp.bfloat16),
        "w_down": (scale_ffn * jax.random.normal(shared_keys[8], (EXPERTS, FFN_DIM, MODEL_DIM), jnp.float32)).astype(jnp.bfloat16),
    }


def rms_norm(rows, gain_vec):
    rows_f = rows.astype(jnp.float32)
    inv_rms = lax.rsqrt(jnp.mean(rows_f * rows_f, axis=-1, keepdims=True) + NORM_EPS)
    return (rows_f * inv_rms * gain_vec.astype(jnp.float32)).astype(jnp.bfloat16)


def attention_block(sequence, attn_gain, w_query, w_key, w_value, w_out):
    normed = rms_norm(sequence, attn_gain).astype(jnp.float32)
    query = jnp.einsum("td,dhe->the", normed, w_query.astype(jnp.float32)).astype(jnp.bfloat16)
    keys = jnp.einsum("td,dhe->the", normed, w_key.astype(jnp.float32)).astype(jnp.bfloat16)
    values = jnp.einsum("td,dhe->the", normed, w_value.astype(jnp.float32)).astype(jnp.bfloat16)
    scores = jnp.einsum("qhe,khe->hqk", query.astype(jnp.float32), keys.astype(jnp.float32)) * (HEAD_DIM ** -0.5)
    causal = jnp.arange(TOKENS)[:, None] >= jnp.arange(TOKENS)[None, :]
    scores = jnp.where(causal[None, :, :], scores, MASK_VALUE)
    attn_prob = jax.nn.softmax(scores, axis=-1).astype(jnp.bfloat16)
    context = jnp.einsum("hqk,khe->qhe", attn_prob.astype(jnp.float32), values.astype(jnp.float32)).astype(jnp.bfloat16)
    attn_out = jnp.einsum("qhe,hed->qd", context.astype(jnp.float32), w_out.astype(jnp.float32))
    return (sequence.astype(jnp.float32) + attn_out).astype(jnp.bfloat16)


def moe_layer(tokens, experts, slots, gates, attn_gain, w_query, w_key, w_value, w_out, moe_gain, w_gate, w_up, w_down):
    residual = lax.map(lambda sequence: attention_block(sequence, attn_gain, w_query, w_key, w_value, w_out), tokens.reshape(GROUP, TOKENS, MODEL_DIM))
    normed = rms_norm(residual, moe_gain).reshape(ROWS, MODEL_DIM)
    row_ids = jnp.arange(ROWS, dtype=jnp.int32)
    owner = row_ids // TOKENS
    buffer_rows = EXPERTS * GROUP * SLOTS
    dest_row = jnp.where(slots >= 0, experts * (GROUP * SLOTS) + owner[:, None] * SLOTS + slots, buffer_rows)
    token_of = jnp.broadcast_to(row_ids[:, None], (ROWS, TOP_K)).reshape(-1)
    source = jnp.full((buffer_rows,), ROWS, jnp.int32).at[dest_row.reshape(-1)].set(token_of, mode="drop")

    def expert_ffn(operands):
        expert_source, gate_w, up_w, down_w = operands
        rows_in = jnp.take(normed, expert_source, axis=0, mode="fill", fill_value=0)
        gate_act = jnp.dot(rows_in, gate_w, preferred_element_type=jnp.float32)
        up_act = jnp.dot(rows_in, up_w, preferred_element_type=jnp.float32)
        hidden = (jax.nn.silu(gate_act) * up_act).astype(jnp.bfloat16)
        return jnp.dot(hidden, down_w, preferred_element_type=jnp.float32).astype(jnp.bfloat16)

    expert_out = lax.map(expert_ffn, (source.reshape(EXPERTS, GROUP * SLOTS), w_gate, w_up, w_down)).reshape(buffer_rows, MODEL_DIM)

    def combine(operands):
        dev_resid, dev_dest, dev_gates = operands
        picked = jnp.take(expert_out, dev_dest, axis=0, mode="fill", fill_value=0).reshape(TOKENS, TOP_K, MODEL_DIM)
        mixed_sum = jnp.einsum("tk,tkd->td", dev_gates.astype(jnp.float32), picked.astype(jnp.float32))
        return (dev_resid.astype(jnp.float32) + mixed_sum).astype(jnp.bfloat16)

    mixed_rows = lax.map(combine, (residual, dest_row.reshape(GROUP, TOKENS * TOP_K), gates.reshape(GROUP, TOKENS, TOP_K)))
    return mixed_rows.reshape(ROWS, MODEL_DIM)


def reference(tokens_a, experts_a, slots_a, gates_a, tokens_b, experts_b, slots_b, gates_b, attn_gain, w_query, w_key, w_value, w_out, moe_gain, w_gate, w_up, w_down):
    out_a = moe_layer(tokens_a, experts_a, slots_a, gates_a, attn_gain, w_query, w_key, w_value, w_out, moe_gain, w_gate, w_up, w_down)
    out_b = moe_layer(tokens_b, experts_b, slots_b, gates_b, attn_gain, w_query, w_key, w_value, w_out, moe_gain, w_gate, w_up, w_down)
    return (out_a, out_b)
```

```python
import functools

import jax
import jax.numpy as jnp
from jax import lax
from jax.experimental import pallas as pl
from jax.experimental.pallas import tpu as pltpu
from jax.sharding import PartitionSpec as P

NORM_EPS = 1e-6
MASK_VALUE = -1e30
MESH = pl.DeviceIdType.MESH
VMEM_LIMIT = 64_000_000


def rms_norm(rows, gain_vec):
    rows_f = rows.astype(jnp.float32)
    inv_rms = lax.rsqrt(jnp.mean(rows_f * rows_f, axis=-1, keepdims=True) + NORM_EPS)
    return (rows_f * inv_rms * gain_vec.astype(jnp.float32)).astype(jnp.bfloat16)


def attention_block(sequence, attn_gain, w_query, w_key, w_value, w_out):
    seq_len = sequence.shape[0]
    normed = rms_norm(sequence, attn_gain)
    query = jnp.einsum("td,dhe->the", normed, w_query, preferred_element_type=jnp.float32).astype(jnp.bfloat16)
    keys = jnp.einsum("td,dhe->the", normed, w_key, preferred_element_type=jnp.float32).astype(jnp.bfloat16)
    values = jnp.einsum("td,dhe->the", normed, w_value, preferred_element_type=jnp.float32).astype(jnp.bfloat16)
    scores = jnp.einsum("qhe,khe->hqk", query, keys, preferred_element_type=jnp.float32) * (w_query.shape[2] ** -0.5)
    causal = lax.broadcasted_iota(jnp.int32, (seq_len, seq_len), 0) >= lax.broadcasted_iota(jnp.int32, (seq_len, seq_len), 1)
    scores = jnp.where(causal[None, :, :], scores, MASK_VALUE)
    attn_prob = jax.nn.softmax(scores, axis=-1).astype(jnp.bfloat16)
    context = jnp.einsum("hqk,khe->qhe", attn_prob, values, preferred_element_type=jnp.float32).astype(jnp.bfloat16)
    attn_out = jnp.einsum("qhe,hed->qd", context, w_out, preferred_element_type=jnp.float32)
    return (sequence.astype(jnp.float32) + attn_out).astype(jnp.bfloat16)


def capacity_of(seq_len, top_k, experts_total):
    return 8 * max(1, (seq_len * top_k) // (4 * experts_total))


def place(group):
    side = int(round((group // 2) ** 0.5))
    me = lax.axis_index("ep")
    return side, lax.rem(me // 2, side), me // (2 * side), lax.rem(me, 2)


def expert_kernel(group, cap, u_hbm, after_hbm, dest_ref, wg_hbm, wu_hbm, wd_hbm, ret_hbm, wg_v, wu_v, wd_v, u_buf, x_buf, h_buf, o_buf, w_sem, u_sem, send_sem, recv_sem):
    local_experts, model_dim, ffn_dim = wg_v.shape
    per_step, seq_len, _ = u_buf.shape
    top_k = dest_ref.shape[1]
    block_rows = local_experts * cap
    half_dim = model_dim // 2
    steps = group // per_step
    f_tile = min(512, ffn_dim)
    n_tile = min(512, half_dim)
    side, my_x, my_y, my_core = place(group)
    line = 2 * side
    me = my_y * line + my_x * 2 + my_core
    mine = (my_y * 2 + my_core, my_x * 2 + my_core)

    def target(step, g):
        late = step // side
        i = lax.rem(step, side)
        if g < 2:
            dx, dy = i, 1 - late
        else:
            dx, dy = (1 - late) * (side - i) + late * (i + 2), 3 - late
        return lax.rem(my_x + dx, side), lax.rem(my_y + dy, side), g % 2

    def load(step, g):
        to_x, to_y, core = target(step, g)
        start = pl.multiple_of((to_y * line + to_x * 2 + core) * seq_len, seq_len)
        return pltpu.make_async_copy(u_hbm.at[pl.ds(start, seq_len)], u_buf.at[g], u_sem.at[g])

    def relay(step, g, half):
        to_x, to_y, core = target(step, g)
        return to_y * line + my_x * 2 + core if half == 0 else my_y * line + to_x * 2 + core

    def landing(step, g, half):
        to_x, to_y, _ = target(step, g)
        return ret_hbm.at[half, to_y if half else to_x, mine[half]]

    def send(step, g, half, slot):
        to_x, to_y, _ = target(step, g)
        return pltpu.make_async_remote_copy(
            src_ref=o_buf.at[slot, half, g],
            dst_ref=landing(step, g, half),
            send_sem=send_sem.at[slot, half, g],
            recv_sem=recv_sem.at[half, to_y if half else to_x, mine[half]],
            device_id={"ep": relay(step, g, half)},
            device_id_type=MESH,
        )

    def keep(step, g, half, slot):
        return pltpu.make_async_copy(o_buf.at[slot, half, g], landing(step, g, half), send_sem.at[slot, half, g])

    def start_out(step, slot):
        for g in range(per_step):
            for half in range(2):

                @pl.when(relay(step, g, half) == me)
                def _():
                    keep(step, g, half, slot).start()

                @pl.when(relay(step, g, half) != me)
                def _():
                    send(step, g, half, slot).start()

    def wait_out(step, slot):
        for g in range(per_step):
            for half in range(2):

                @pl.when(relay(step, g, half) == me)
                def _():
                    keep(step, g, half, slot).wait()

                @pl.when(relay(step, g, half) != me)
                def _():
                    send(step, g, half, slot).wait_send()

    weights = [pltpu.make_async_copy(a, b, w_sem.at[i]) for i, (a, b) in enumerate(((wg_hbm, wg_v), (wu_hbm, wu_v), (wd_hbm, wd_v)))]
    for g in range(per_step):
        load(0, g).start()
    for w in weights:
        w.start()

    barrier = pltpu.get_barrier_semaphore()

    @pl.loop(1, line)
    def _(k):
        j = lax.rem(mine[0] + k, line)
        pl.semaphore_signal(barrier, inc=1, device_id={"ep": (j // 2) * line + my_x * 2 + lax.rem(j, 2)}, device_id_type=MESH)
        j = lax.rem(mine[1] + k, line)
        pl.semaphore_signal(barrier, inc=1, device_id={"ep": my_y * line + j}, device_id_type=MESH)

    pl.semaphore_wait(barrier, 2 * (line - 1))
    for w in weights:
        w.wait()

    row_id = (me * block_rows + lax.broadcasted_iota(jnp.int32, (block_rows, seq_len), 0)).astype(jnp.float32)

    @pl.loop(0, steps)
    def _(step):
        slot = lax.rem(step, 2)
        for g in range(per_step):
            load(step, g).wait()
            to_x, to_y, core = target(step, g)
            dest = dest_ref[to_y * line + to_x * 2 + core]
            hit = row_id == dest[0:1, :]
            for j in range(1, top_k):
                hit = hit | (row_id == dest[j : j + 1, :])
            pick = jnp.where(hit, 1.0, 0.0).astype(jnp.bfloat16)
            for n in range(model_dim // n_tile):
                cols = slice(n * n_tile, (n + 1) * n_tile)
                rows = jnp.dot(pick, u_buf[g, :, cols], preferred_element_type=jnp.float32).astype(jnp.bfloat16)
                for e in range(local_experts):
                    x_buf[e, g * cap : (g + 1) * cap, cols] = rows[e * cap : (e + 1) * cap]

            @pl.when(step < steps - 1)
            def _():
                load(step + 1, g).start()

        @pl.when(step >= 2)
        def _():
            wait_out(step - 2, slot)

        for e in range(local_experts):

            @pl.loop(0, ffn_dim // f_tile)
            def _(f):
                cols = pl.ds(pl.multiple_of(f * f_tile, f_tile), f_tile)
                gate_act = jnp.dot(x_buf[e], wg_v[e, :, cols], preferred_element_type=jnp.float32)
                up_act = jnp.dot(x_buf[e], wu_v[e, :, cols], preferred_element_type=jnp.float32)
                h_buf[:, cols] = (gate_act * jax.nn.sigmoid(gate_act) * up_act).astype(jnp.bfloat16)

            for half in range(2):

                @pl.loop(0, half_dim // n_tile)
                def _(n):
                    cols = pl.ds(pl.multiple_of(n * n_tile, n_tile), n_tile)
                    w_cols = pl.ds(pl.multiple_of(half * half_dim + n * n_tile, n_tile), n_tile)
                    rows = jnp.dot(h_buf[...], wd_v[e, :, w_cols], preferred_element_type=jnp.float32).astype(jnp.bfloat16)
                    for g in range(per_step):
                        o_buf[slot, half, g, e * cap : (e + 1) * cap, cols] = rows[g * cap : (g + 1) * cap]

        start_out(step, slot)

    for step in range(max(0, steps - 2), steps):
        wait_out(step, step % 2)

    @pl.loop(1, line)
    def _(k):
        for half in range(2):
            j = lax.rem(mine[half] + k, line)
            peer = (j // 2) * line + my_x * 2 + lax.rem(j, 2) if half == 0 else my_y * line + j
            for t in range(side):
                pltpu.make_async_remote_copy(
                    src_ref=o_buf.at[0, half, 0],
                    dst_ref=ret_hbm.at[half, t, j],
                    send_sem=send_sem.at[0, half, 0],
                    recv_sem=recv_sem.at[half, t, j],
                    device_id={"ep": peer},
                    device_id_type=MESH,
                ).wait_recv()


def experts_to_relays(gathered, after, dest_all, w_gate, w_up, w_down, group, cap):
    local_experts, model_dim, ffn_dim = w_gate.shape
    seq_len = gathered.shape[0] // group
    side = int(round((group // 2) ** 0.5))
    per_step = 4
    rows = group * local_experts * cap
    hbm = pl.BlockSpec(memory_space=pl.ANY)
    return pl.pallas_call(
        functools.partial(expert_kernel, group, cap),
        out_shape=jax.ShapeDtypeStruct((2, side, 2 * side, local_experts * cap, model_dim // 2), jnp.bfloat16),
        in_specs=[hbm, hbm, pl.BlockSpec(memory_space=pltpu.VMEM), hbm, hbm, hbm],
        out_specs=hbm,
        scratch_shapes=[
            pltpu.VMEM(w_gate.shape, jnp.bfloat16),
            pltpu.VMEM(w_up.shape, jnp.bfloat16),
            pltpu.VMEM(w_down.shape, jnp.bfloat16),
            pltpu.VMEM((per_step, seq_len, model_dim), jnp.bfloat16),
            pltpu.VMEM((local_experts, per_step * cap, model_dim), jnp.bfloat16),
            pltpu.VMEM((per_step * cap, ffn_dim), jnp.bfloat16),
            pltpu.VMEM((2, 2, per_step, local_experts * cap, model_dim // 2), jnp.bfloat16),
            pltpu.SemaphoreType.DMA((3,)),
            pltpu.SemaphoreType.DMA((per_step,)),
            pltpu.SemaphoreType.DMA((2, 2, per_step)),
            pltpu.SemaphoreType.DMA((2, side, 2 * side)),
        ],
        compiler_params=pltpu.CompilerParams(collective_id=0, has_side_effects=True, vmem_limit_bytes=VMEM_LIMIT),
        cost_estimate=pl.CostEstimate(flops=2 * rows * model_dim * (3 * ffn_dim + seq_len), bytes_accessed=200_000_000, transcendentals=0),
        name="experts_to_relays",
    )(gathered, after, dest_all, w_gate, w_up, w_down)


def relay_kernel(group, ret_hbm, dest_ref, gates_ref, part_hbm, r_buf, w_buf, p_buf, r_sem, send_sem, recv_sem):
    side, my_x, my_y, my_core = place(group)
    line = 2 * side
    _, block_rows, half_dim = r_buf.shape[1:]
    n_tile = min(512, half_dim)
    mine = (my_x, my_y)

    def target(i, half):
        return lax.rem(mine[half] + side - 1 - i, side)

    def device(half, t):
        return my_y * line + t * 2 + my_core if half == 0 else t * line + my_x * 2 + my_core

    def load(i, half):
        return pltpu.make_async_copy(ret_hbm.at[half, target(i, half)], r_buf.at[half], r_sem.at[half])

    def send(i, half):
        return pltpu.make_async_remote_copy(
            src_ref=p_buf.at[i, half],
            dst_ref=part_hbm.at[half, mine[half]],
            send_sem=send_sem.at[i, half],
            recv_sem=recv_sem.at[half, mine[half]],
            device_id={"ep": device(half, target(i, half))},
            device_id_type=MESH,
        )

    def keep(half):
        return pltpu.make_async_copy(p_buf.at[side - 1, half], part_hbm.at[half, mine[half]], send_sem.at[side - 1, half])

    for half in range(2):
        load(0, half).start()

    barrier = pltpu.get_barrier_semaphore()
    for half in range(2):
        for k in range(1, side):
            pl.semaphore_signal(barrier, inc=1, device_id={"ep": device(half, lax.rem(mine[half] + k, side))}, device_id_type=MESH)
    pl.semaphore_wait(barrier, 2 * (side - 1))

    seq_len, top_k = dest_ref.shape[1:]
    lane = lax.broadcasted_iota(jnp.int32, (seq_len, block_rows), 1)

    @pl.loop(0, side)
    def _(i):
        for half in range(2):
            t = target(i, half)
            dest = dest_ref[half * side + t]
            gates = gates_ref[half * side + t]
            for j in range(line):
                owner = (j // 2) * line + my_x * 2 + j % 2 if half == 0 else my_y * line + j
                row_id = (owner * block_rows + lane).astype(jnp.float32)
                mix = jnp.zeros((seq_len, block_rows), jnp.float32)
                for k in range(top_k):
                    mix = jnp.where(dest[:, k : k + 1] == row_id, gates[:, k : k + 1], mix)
                w_buf[:, j * block_rows : (j + 1) * block_rows] = mix.astype(jnp.bfloat16)
            load(i, half).wait()
            for n in range(half_dim // n_tile):
                cols = slice(n * n_tile, (n + 1) * n_tile)
                rows = r_buf[half, :, :, cols].reshape(line * block_rows, n_tile)
                p_buf[i, half, :, cols] = jnp.dot(w_buf[...], rows, preferred_element_type=jnp.float32)

            @pl.when(i < side - 1)
            def _():
                load(i + 1, half).start()
                send(i, half).start()

            @pl.when(i == side - 1)
            def _():
                keep(half).start()

    for half in range(2):
        keep(half).wait()
        for i in range(side - 1):
            send(i, half).wait_send()
        for k in range(1, side):
            j = lax.rem(mine[half] + k, side)
            pltpu.make_async_remote_copy(
                src_ref=p_buf.at[0, half],
                dst_ref=part_hbm.at[half, j],
                send_sem=send_sem.at[0, half],
                recv_sem=recv_sem.at[half, j],
                device_id={"ep": device(half, j)},
                device_id_type=MESH,
            ).wait_recv()


def relay_sums(ret, dest, gates, group):
    _, side, line, block_rows, half_dim = ret.shape
    seq_len = dest.shape[1]
    hbm = pl.BlockSpec(memory_space=pl.ANY)
    vmem = pl.BlockSpec(memory_space=pltpu.VMEM)
    return pl.pallas_call(
        functools.partial(relay_kernel, group),
        out_shape=jax.ShapeDtypeStruct((2, side, seq_len, half_dim), jnp.float32),
        in_specs=[hbm, vmem, vmem],
        out_specs=hbm,
        scratch_shapes=[
            pltpu.VMEM((2, line, block_rows, half_dim), jnp.bfloat16),
            pltpu.VMEM((seq_len, line * block_rows), jnp.bfloat16),
            pltpu.VMEM((side, 2, seq_len, half_dim), jnp.float32),
            pltpu.SemaphoreType.DMA((2,)),
            pltpu.SemaphoreType.DMA((side, 2)),
            pltpu.SemaphoreType.DMA((2, side)),
        ],
        compiler_params=pltpu.CompilerParams(collective_id=1, has_side_effects=True, vmem_limit_bytes=VMEM_LIMIT),
        cost_estimate=pl.CostEstimate(flops=2 * seq_len * ret.size, bytes_accessed=2 * ret.size + 8 * side * seq_len * half_dim, transcendentals=0),
        name="relay_sums",
    )(ret, dest, gates)


def final_kernel(resid_ref, part_ref, out_ref):
    total = resid_ref[...].astype(jnp.float32)
    for i in range(part_ref.shape[1]):
        total = total + part_ref[0, i]
    out_ref[...] = total.astype(out_ref.dtype)


def final_sum(residual, part):
    seq_len, model_dim = residual.shape
    side, half_dim = part.shape[1], part.shape[3]
    tile = min(128, seq_len)
    return pl.pallas_call(
        final_kernel,
        grid=(2, seq_len // tile),
        out_shape=jax.ShapeDtypeStruct(residual.shape, residual.dtype),
        in_specs=[pl.BlockSpec((tile, half_dim), lambda h, r: (r, h)), pl.BlockSpec((1, side, tile, half_dim), lambda h, r: (h, 0, r, 0))],
        out_specs=pl.BlockSpec((tile, half_dim), lambda h, r: (r, h)),
        cost_estimate=pl.CostEstimate(flops=part.size, bytes_accessed=4 * part.size + 4 * residual.size, transcendentals=0),
        name="final_sum",
    )(residual, part)


def solution(mesh):
    group = mesh.shape["ep"]
    row_spec = P(("dp", "ep"), None)
    full_spec = P(None, None, None)
    gain_spec = P(None)
    expert_spec = P("ep", None, None)
    in_specs = (row_spec, row_spec, row_spec, row_spec, row_spec, row_spec, row_spec, row_spec, gain_spec, full_spec, full_spec, full_spec, full_spec, gain_spec, expert_spec, expert_spec, expert_spec)

    def device_fn(tokens_a, experts_a, slots_a, gates_a, tokens_b, experts_b, slots_b, gates_b, attn_gain, w_query, w_key, w_value, w_out, moe_gain, w_gate, w_up, w_down):
        seq_len, top_k = experts_a.shape
        cap = capacity_of(seq_len, top_k, w_gate.shape[0] * group)
        dest_a = jnp.where(slots_a >= 0, experts_a * cap + slots_a, -1)
        dest_b = jnp.where(slots_b >= 0, experts_b * cap + slots_b, -1)
        table = jnp.stack([v.T.astype(jnp.float32) for v in (dest_a, gates_a, dest_b, gates_b)])
        table = lax.all_gather(table, "ep")
        side, my_x, my_y, my_core = place(group)
        grid = table.reshape((side, side, 2) + table.shape[1:])
        grid = lax.dynamic_index_in_dim(grid, my_core, 2, keepdims=False)
        lines = jnp.concatenate([lax.dynamic_index_in_dim(grid, my_y, 0, keepdims=False), lax.dynamic_index_in_dim(grid, my_x, 1, keepdims=False)])
        lines = jnp.swapaxes(lines, 2, 3)

        resid_a = attention_block(tokens_a, attn_gain, w_query, w_key, w_value, w_out)
        normed_a = rms_norm(resid_a, moe_gain)
        gathered_a = lax.all_gather(normed_a, "ep", tiled=True)
        tokens_b, normed_a = lax.optimization_barrier((tokens_b, normed_a))
        resid_b = attention_block(tokens_b, attn_gain, w_query, w_key, w_value, w_out)
        normed_b = rms_norm(resid_b, moe_gain)
        gathered_b = lax.all_gather(normed_b, "ep", tiled=True)

        returned_a = experts_to_relays(gathered_a, normed_b, table[:, 0], w_gate, w_up, w_down, group, cap)
        part_a = relay_sums(returned_a, lines[:, 0], lines[:, 1], group)
        out_a = final_sum(resid_a, part_a)
        returned_b = experts_to_relays(gathered_b, out_a, table[:, 2], w_gate, w_up, w_down, group, cap)
        part_b = relay_sums(returned_b, lines[:, 2], lines[:, 3], group)
        return out_a, final_sum(resid_b, part_b)

    return jax.shard_map(device_fn, mesh=mesh, in_specs=in_specs, out_specs=(row_spec, row_spec), check_vma=False)
```

```python
import functools

import jax
import jax.numpy as jnp
from jax import lax
from jax.experimental import pallas as pl
from jax.experimental.pallas import tpu as pltpu
from jax.sharding import PartitionSpec as P

NORM_EPS = 1e-6
MASK_VALUE = -1e30
MESH = pl.DeviceIdType.MESH
VMEM_LIMIT = 64_000_000
SLOTS_OUT = 4


def rms_norm(rows, gain_vec):
    rows_f = rows.astype(jnp.float32)
    inv_rms = lax.rsqrt(jnp.mean(rows_f * rows_f, axis=-1, keepdims=True) + NORM_EPS)
    return (rows_f * inv_rms * gain_vec.astype(jnp.float32)).astype(jnp.bfloat16)


def attention_block(sequence, attn_gain, w_query, w_key, w_value, w_out):
    seq_len = sequence.shape[0]
    normed = rms_norm(sequence, attn_gain)
    query = jnp.einsum("td,dhe->the", normed, w_query, preferred_element_type=jnp.float32).astype(jnp.bfloat16)
    keys = jnp.einsum("td,dhe->the", normed, w_key, preferred_element_type=jnp.float32).astype(jnp.bfloat16)
    values = jnp.einsum("td,dhe->the", normed, w_value, preferred_element_type=jnp.float32).astype(jnp.bfloat16)
    scores = jnp.einsum("qhe,khe->hqk", query, keys, preferred_element_type=jnp.float32) * (w_query.shape[2] ** -0.5)
    causal = lax.broadcasted_iota(jnp.int32, (seq_len, seq_len), 0) >= lax.broadcasted_iota(jnp.int32, (seq_len, seq_len), 1)
    scores = jnp.where(causal[None, :, :], scores, MASK_VALUE)
    attn_prob = jax.nn.softmax(scores, axis=-1).astype(jnp.bfloat16)
    context = jnp.einsum("hqk,khe->qhe", attn_prob, values, preferred_element_type=jnp.float32).astype(jnp.bfloat16)
    attn_out = jnp.einsum("qhe,hed->qd", context, w_out, preferred_element_type=jnp.float32)
    return (sequence.astype(jnp.float32) + attn_out).astype(jnp.bfloat16)


def capacity_of(seq_len, top_k, experts_total):
    return 8 * max(1, (seq_len * top_k) // (4 * experts_total))


def place(group):
    side = int(round((group // 2) ** 0.5))
    me = lax.axis_index("ep")
    return side, lax.rem(me // 2, side), me // (2 * side), lax.rem(me, 2)


def expert_kernel(group, cap, u_hbm, after_hbm, dest_ref, wg_hbm, wu_hbm, wd_hbm, ret_hbm, wg_v, wu_v, wd_v, u_buf, x_buf, h_buf, o_buf, w_sem, u_sem, send_sem, recv_sem):
    local_experts, model_dim, ffn_dim = wg_v.shape
    per_step, seq_len, _ = u_buf.shape
    top_k = dest_ref.shape[1]
    block_rows = local_experts * cap
    half_dim = model_dim // 2
    steps = group // per_step
    slots = o_buf.shape[0]
    f_tile = min(512, ffn_dim)
    n_tile = min(512, half_dim)
    side, my_x, my_y, my_core = place(group)
    line = 2 * side
    me = my_y * line + my_x * 2 + my_core
    mine = (my_y * 2 + my_core, my_x * 2 + my_core)

    def target(step, g):
        late = step // side
        i = lax.rem(step, side)
        if g < 2:
            dx, dy = i, 1 - late
        else:
            dx, dy = i + side // 2, 3 - late
        return lax.rem(my_x + dx, side), lax.rem(my_y + dy, side), g % 2

    def load(step, g):
        to_x, to_y, core = target(step, g)
        start = pl.multiple_of((to_y * line + to_x * 2 + core) * seq_len, seq_len)
        return pltpu.make_async_copy(u_hbm.at[pl.ds(start, seq_len)], u_buf.at[g], u_sem.at[g])

    def relay(step, g, half):
        to_x, to_y, core = target(step, g)
        return to_y * line + my_x * 2 + core if half == 0 else my_y * line + to_x * 2 + core

    def landing(step, g, half):
        to_x, to_y, _ = target(step, g)
        return ret_hbm.at[half, to_y if half else to_x, mine[half]]

    def send(step, g, half, slot):
        to_x, to_y, _ = target(step, g)
        return pltpu.make_async_remote_copy(
            src_ref=o_buf.at[slot, half, g],
            dst_ref=landing(step, g, half),
            send_sem=send_sem.at[slot, half, g],
            recv_sem=recv_sem.at[half, to_y if half else to_x, mine[half]],
            device_id={"ep": relay(step, g, half)},
            device_id_type=MESH,
        )

    def keep(step, g, half, slot):
        return pltpu.make_async_copy(o_buf.at[slot, half, g], landing(step, g, half), send_sem.at[slot, half, g])

    def start_out(step, slot):
        for g in range(per_step):
            for half in range(2):

                @pl.when(relay(step, g, half) == me)
                def _():
                    keep(step, g, half, slot).start()

                @pl.when(relay(step, g, half) != me)
                def _():
                    send(step, g, half, slot).start()

    def wait_out(step, slot):
        for g in range(per_step):
            for half in range(2):

                @pl.when(relay(step, g, half) == me)
                def _():
                    keep(step, g, half, slot).wait()

                @pl.when(relay(step, g, half) != me)
                def _():
                    send(step, g, half, slot).wait_send()

    weights = [pltpu.make_async_copy(a, b, w_sem.at[i]) for i, (a, b) in enumerate(((wg_hbm, wg_v), (wu_hbm, wu_v), (wd_hbm, wd_v)))]
    for g in range(per_step):
        load(0, g).start()
    for w in weights:
        w.start()

    barrier = pltpu.get_barrier_semaphore()

    @pl.loop(1, line)
    def _(k):
        j = lax.rem(mine[0] + k, line)
        pl.semaphore_signal(barrier, inc=1, device_id={"ep": (j // 2) * line + my_x * 2 + lax.rem(j, 2)}, device_id_type=MESH)
        j = lax.rem(mine[1] + k, line)
        pl.semaphore_signal(barrier, inc=1, device_id={"ep": my_y * line + j}, device_id_type=MESH)

    pl.semaphore_wait(barrier, 2 * (line - 1))
    for w in weights:
        w.wait()

    row_id = (me * block_rows + lax.broadcasted_iota(jnp.int32, (block_rows, seq_len), 0)).astype(jnp.float32)

    @pl.loop(0, steps)
    def _(step):
        slot = lax.rem(step, slots)
        for g in range(per_step):
            load(step, g).wait()
            to_x, to_y, core = target(step, g)
            dest = dest_ref[to_y * line + to_x * 2 + core]
            hit = row_id == dest[0:1, :]
            for j in range(1, top_k):
                hit = hit | (row_id == dest[j : j + 1, :])
            pick = jnp.where(hit, 1.0, 0.0).astype(jnp.bfloat16)
            for n in range(model_dim // n_tile):
                cols = slice(n * n_tile, (n + 1) * n_tile)
                rows = jnp.dot(pick, u_buf[g, :, cols], preferred_element_type=jnp.float32).astype(jnp.bfloat16)
                for e in range(local_experts):
                    x_buf[e, g * cap : (g + 1) * cap, cols] = rows[e * cap : (e + 1) * cap]

            @pl.when(step < steps - 1)
            def _():
                load(step + 1, g).start()

        @pl.when(step >= slots)
        def _():
            wait_out(step - slots, slot)

        for e in range(local_experts):

            @pl.loop(0, ffn_dim // f_tile)
            def _(f):
                cols = pl.ds(pl.multiple_of(f * f_tile, f_tile), f_tile)
                gate_act = jnp.dot(x_buf[e], wg_v[e, :, cols], preferred_element_type=jnp.float32)
                up_act = jnp.dot(x_buf[e], wu_v[e, :, cols], preferred_element_type=jnp.float32)
                h_buf[:, cols] = (gate_act * jax.nn.sigmoid(gate_act) * up_act).astype(jnp.bfloat16)

            for half in range(2):

                @pl.loop(0, half_dim // n_tile)
                def _(n):
                    cols = pl.ds(pl.multiple_of(n * n_tile, n_tile), n_tile)
                    w_cols = pl.ds(pl.multiple_of(half * half_dim + n * n_tile, n_tile), n_tile)
                    rows = jnp.dot(h_buf[...], wd_v[e, :, w_cols], preferred_element_type=jnp.float32).astype(jnp.bfloat16)
                    for g in range(per_step):
                        o_buf[slot, half, g, e * cap : (e + 1) * cap, cols] = rows[g * cap : (g + 1) * cap]

        start_out(step, slot)

    @pl.loop(max(0, steps - slots), steps)
    def _(step):
        wait_out(step, lax.rem(step, slots))

    @pl.loop(1, line)
    def _(k):
        for half in range(2):
            j = lax.rem(mine[half] + k, line)
            peer = (j // 2) * line + my_x * 2 + lax.rem(j, 2) if half == 0 else my_y * line + j
            for t in range(side):
                pltpu.make_async_remote_copy(
                    src_ref=o_buf.at[0, half, 0],
                    dst_ref=ret_hbm.at[half, t, j],
                    send_sem=send_sem.at[0, half, 0],
                    recv_sem=recv_sem.at[half, t, j],
                    device_id={"ep": peer},
                    device_id_type=MESH,
                ).wait_recv()


def experts_to_relays(gathered, after, dest_all, w_gate, w_up, w_down, group, cap):
    local_experts, model_dim, ffn_dim = w_gate.shape
    seq_len = gathered.shape[0] // group
    side = int(round((group // 2) ** 0.5))
    per_step = 4
    rows = group * local_experts * cap
    hbm = pl.BlockSpec(memory_space=pl.ANY)
    return pl.pallas_call(
        functools.partial(expert_kernel, group, cap),
        out_shape=jax.ShapeDtypeStruct((2, side, 2 * side, local_experts * cap, model_dim // 2), jnp.bfloat16),
        in_specs=[hbm, hbm, pl.BlockSpec(memory_space=pltpu.VMEM), hbm, hbm, hbm],
        out_specs=hbm,
        scratch_shapes=[
            pltpu.VMEM(w_gate.shape, jnp.bfloat16),
            pltpu.VMEM(w_up.shape, jnp.bfloat16),
            pltpu.VMEM(w_down.shape, jnp.bfloat16),
            pltpu.VMEM((per_step, seq_len, model_dim), jnp.bfloat16),
            pltpu.VMEM((local_experts, per_step * cap, model_dim), jnp.bfloat16),
            pltpu.VMEM((per_step * cap, ffn_dim), jnp.bfloat16),
            pltpu.VMEM((SLOTS_OUT, 2, per_step, local_experts * cap, model_dim // 2), jnp.bfloat16),
            pltpu.SemaphoreType.DMA((3,)),
            pltpu.SemaphoreType.DMA((per_step,)),
            pltpu.SemaphoreType.DMA((SLOTS_OUT, 2, per_step)),
            pltpu.SemaphoreType.DMA((2, side, 2 * side)),
        ],
        compiler_params=pltpu.CompilerParams(collective_id=0, has_side_effects=True, vmem_limit_bytes=VMEM_LIMIT),
        cost_estimate=pl.CostEstimate(flops=2 * rows * model_dim * (3 * ffn_dim + seq_len), bytes_accessed=200_000_000, transcendentals=0),
        name="experts_to_relays",
    )(gathered, after, dest_all, w_gate, w_up, w_down)


def relay_kernel(group, ret_hbm, dest_ref, gates_ref, part_hbm, r_buf, w_buf, p_buf, r_sem, send_sem, recv_sem):
    side, my_x, my_y, my_core = place(group)
    line = 2 * side
    _, block_rows, half_dim = r_buf.shape[1:]
    n_tile = min(512, half_dim)
    mine = (my_x, my_y)

    def target(i, half):
        return lax.rem(mine[half] + side - 1 - i, side)

    def device(half, t):
        return my_y * line + t * 2 + my_core if half == 0 else t * line + my_x * 2 + my_core

    def load(i, half):
        return pltpu.make_async_copy(ret_hbm.at[half, target(i, half)], r_buf.at[half], r_sem.at[half])

    def send(i, half):
        return pltpu.make_async_remote_copy(
            src_ref=p_buf.at[i, half],
            dst_ref=part_hbm.at[half, mine[half]],
            send_sem=send_sem.at[i, half],
            recv_sem=recv_sem.at[half, mine[half]],
            device_id={"ep": device(half, target(i, half))},
            device_id_type=MESH,
        )

    def keep(half):
        return pltpu.make_async_copy(p_buf.at[side - 1, half], part_hbm.at[half, mine[half]], send_sem.at[side - 1, half])

    for half in range(2):
        load(0, half).start()

    barrier = pltpu.get_barrier_semaphore()
    for half in range(2):
        for k in range(1, side):
            pl.semaphore_signal(barrier, inc=1, device_id={"ep": device(half, lax.rem(mine[half] + k, side))}, device_id_type=MESH)
    pl.semaphore_wait(barrier, 2 * (side - 1))

    seq_len, top_k = dest_ref.shape[1:]
    lane = lax.broadcasted_iota(jnp.int32, (seq_len, block_rows), 1)

    @pl.loop(0, side)
    def _(i):
        for half in range(2):
            t = target(i, half)
            dest = dest_ref[half * side + t]
            gates = gates_ref[half * side + t]
            for j in range(line):
                owner = (j // 2) * line + my_x * 2 + j % 2 if half == 0 else my_y * line + j
                row_id = (owner * block_rows + lane).astype(jnp.float32)
                mix = jnp.zeros((seq_len, block_rows), jnp.float32)
                for k in range(top_k):
                    mix = jnp.where(dest[:, k : k + 1] == row_id, gates[:, k : k + 1], mix)
                w_buf[:, j * block_rows : (j + 1) * block_rows] = mix.astype(jnp.bfloat16)
            load(i, half).wait()
            for n in range(half_dim // n_tile):
                cols = slice(n * n_tile, (n + 1) * n_tile)
                rows = r_buf[half, :, :, cols].reshape(line * block_rows, n_tile)
                p_buf[i, half, :, cols] = jnp.dot(w_buf[...], rows, preferred_element_type=jnp.float32)

            @pl.when(i < side - 1)
            def _():
                load(i + 1, half).start()
                send(i, half).start()

            @pl.when(i == side - 1)
            def _():
                keep(half).start()

    for half in range(2):
        keep(half).wait()
        for i in range(side - 1):
            send(i, half).wait_send()
        for k in range(1, side):
            j = lax.rem(mine[half] + k, side)
            pltpu.make_async_remote_copy(
                src_ref=p_buf.at[0, half],
                dst_ref=part_hbm.at[half, j],
                send_sem=send_sem.at[0, half],
                recv_sem=recv_sem.at[half, j],
                device_id={"ep": device(half, j)},
                device_id_type=MESH,
            ).wait_recv()


def relay_sums(ret, dest, gates, group):
    _, side, line, block_rows, half_dim = ret.shape
    seq_len = dest.shape[1]
    hbm = pl.BlockSpec(memory_space=pl.ANY)
    vmem = pl.BlockSpec(memory_space=pltpu.VMEM)
    return pl.pallas_call(
        functools.partial(relay_kernel, group),
        out_shape=jax.ShapeDtypeStruct((2, side, seq_len, half_dim), jnp.float32),
        in_specs=[hbm, vmem, vmem],
        out_specs=hbm,
        scratch_shapes=[
            pltpu.VMEM((2, line, block_rows, half_dim), jnp.bfloat16),
            pltpu.VMEM((seq_len, line * block_rows), jnp.bfloat16),
            pltpu.VMEM((side, 2, seq_len, half_dim), jnp.float32),
            pltpu.SemaphoreType.DMA((2,)),
            pltpu.SemaphoreType.DMA((side, 2)),
            pltpu.SemaphoreType.DMA((2, side)),
        ],
        compiler_params=pltpu.CompilerParams(collective_id=1, has_side_effects=True, vmem_limit_bytes=VMEM_LIMIT),
        cost_estimate=pl.CostEstimate(flops=2 * seq_len * ret.size, bytes_accessed=2 * ret.size + 8 * side * seq_len * half_dim, transcendentals=0),
        name="relay_sums",
    )(ret, dest, gates)


def final_kernel(resid_ref, part_ref, out_ref):
    total = resid_ref[...].astype(jnp.float32)
    for i in range(part_ref.shape[1]):
        total = total + part_ref[0, i]
    out_ref[...] = total.astype(out_ref.dtype)


def final_sum(residual, part):
    seq_len, model_dim = residual.shape
    side, half_dim = part.shape[1], part.shape[3]
    tile = min(128, seq_len)
    return pl.pallas_call(
        final_kernel,
        grid=(2, seq_len // tile),
        out_shape=jax.ShapeDtypeStruct(residual.shape, residual.dtype),
        in_specs=[pl.BlockSpec((tile, half_dim), lambda h, r: (r, h)), pl.BlockSpec((1, side, tile, half_dim), lambda h, r: (h, 0, r, 0))],
        out_specs=pl.BlockSpec((tile, half_dim), lambda h, r: (r, h)),
        cost_estimate=pl.CostEstimate(flops=part.size, bytes_accessed=4 * part.size + 4 * residual.size, transcendentals=0),
        name="final_sum",
    )(residual, part)


def solution(mesh):
    group = mesh.shape["ep"]
    row_spec = P(("dp", "ep"), None)
    full_spec = P(None, None, None)
    gain_spec = P(None)
    expert_spec = P("ep", None, None)
    in_specs = (row_spec, row_spec, row_spec, row_spec, row_spec, row_spec, row_spec, row_spec, gain_spec, full_spec, full_spec, full_spec, full_spec, gain_spec, expert_spec, expert_spec, expert_spec)

    def device_fn(tokens_a, experts_a, slots_a, gates_a, tokens_b, experts_b, slots_b, gates_b, attn_gain, w_query, w_key, w_value, w_out, moe_gain, w_gate, w_up, w_down):
        seq_len, top_k = experts_a.shape
        cap = capacity_of(seq_len, top_k, w_gate.shape[0] * group)
        dest_a = jnp.where(slots_a >= 0, experts_a * cap + slots_a, -1)
        dest_b = jnp.where(slots_b >= 0, experts_b * cap + slots_b, -1)
        table = jnp.stack([v.T.astype(jnp.float32) for v in (dest_a, gates_a, dest_b, gates_b)])
        table = lax.all_gather(table, "ep")
        side, my_x, my_y, my_core = place(group)
        grid = table.reshape((side, side, 2) + table.shape[1:])
        grid = lax.dynamic_index_in_dim(grid, my_core, 2, keepdims=False)
        lines = jnp.concatenate([lax.dynamic_index_in_dim(grid, my_y, 0, keepdims=False), lax.dynamic_index_in_dim(grid, my_x, 1, keepdims=False)])
        lines = jnp.swapaxes(lines, 2, 3)

        resid_a = attention_block(tokens_a, attn_gain, w_query, w_key, w_value, w_out)
        normed_a = rms_norm(resid_a, moe_gain)
        gathered_a = lax.all_gather(normed_a, "ep", tiled=True)
        tokens_b, normed_a = lax.optimization_barrier((tokens_b, normed_a))
        resid_b = attention_block(tokens_b, attn_gain, w_query, w_key, w_value, w_out)
        normed_b = rms_norm(resid_b, moe_gain)
        gathered_b = lax.all_gather(normed_b, "ep", tiled=True)

        returned_a = experts_to_relays(gathered_a, normed_b, table[:, 0], w_gate, w_up, w_down, group, cap)
        part_a = relay_sums(returned_a, lines[:, 0], lines[:, 1], group)
        out_a = final_sum(resid_a, part_a)
        returned_b = experts_to_relays(gathered_b, out_a, table[:, 2], w_gate, w_up, w_down, group, cap)
        part_b = relay_sums(returned_b, lines[:, 2], lines[:, 3], group)
        return out_a, final_sum(resid_b, part_b)

    return jax.shard_map(device_fn, mesh=mesh, in_specs=in_specs, out_specs=(row_spec, row_spec), check_vma=False)
```
